32 devices in a mesh: slab: 2 (over x), py: 4 (over y, core), px: 4 (over z).
Axes of the slice: x: 2, y: 2, z: 4, core: 2. Of those that a mesh axis runs over, the one named last changes fastest.
Arguments:
- state: bfloat16 [2, 3, 16, 1024, 1024], P(None, None, 'slab', ('py', 'px')), may hold values from -12 to 12
- shells: int32 [16, 1024, 1024], P('slab', ('py', 'px')), may hold values from 0 to 511
Outputs:
- restored: float32 [2, 3, 16, 1024, 1024], P(None, None, ('slab', 'py'), None, 'px')
- spectrum: float32 [512], replicated
The draws below stay inside these ranges and needn't reach their ends.
All inputs are finite; a program needn't handle non-finite values.
Results may differ from the reference program's by a relative error of at most 0.0003.
Values may be sent and summed in bfloat16 or wider, within the bound.
A program may use at most 128 MiB of HBM per device.

```python
import math
import jax
import jax.numpy as jnp

X = 1024
Y = 1024
SHELLS = 512
Z = 16


def integer_root(squares):
    root = jnp.zeros_like(squares)
    for level in range(11, -1, -1):
        candidate = root + (1 << level)
        root = jnp.where(candidate * candidate <= squares, candidate, root)
    return root


def centred(count, key):
    spread = count // 8
    centre = count // 2 + jax.random.randint(key, (), -spread, spread + 1, jnp.int32)
    offsets = jnp.arange(count, dtype=jnp.int32) - centre
    reach = jnp.maximum(centre, count - 1 - centre)
    return (offsets, reach)


def shell_labels(key):
    base_key = jax.random.fold_in(key, 29)
    plane_key, row_key, column_key, jitter_key = jax.random.split(base_key, 4)
    plane_off, plane_reach = centred(Z, plane_key)
    row_off, row_reach = centred(Y, row_key)
    column_off, column_reach = centred(X, column_key)
    squares = (plane_off * plane_off)[:, None, None] + (row_off * row_off)[None, :, None] + (column_off * column_off)[None, None, :]
    radius = integer_root(squares)
    outer = integer_root(plane_reach * plane_reach + row_reach * row_reach + column_reach * column_reach)
    labels = radius * SHELLS // (outer + 1)
    jitter = jax.random.randint(jitter_key, (Z, Y, X), 0, 2, jnp.int32)
    return jnp.minimum(labels + jitter, SHELLS - 1).astype(jnp.int32)


def draw_shells(key, part):
    return shell_labels(key)


def draw_state(key, part):
    labels = shell_labels(key)
    first_key = jax.random.fold_in(jax.random.fold_in(key, 11), 0)
    column_key = jax.random.fold_in(jax.random.fold_in(key, 11), 2)
    row_key = jax.random.fold_in(jax.random.fold_in(key, 11), 3)
    decay = 1.0 / jnp.sqrt(1.0 + labels.astype(jnp.float32))
    column_gain = jnp.exp(jax.random.uniform(column_key, (X,), jnp.float32, math.log(0.5), math.log(2.0)))
    row_gain = jnp.exp(jax.random.uniform(row_key, (Y,), jnp.float32, math.log(0.7), math.log(1.4)))
    amplitude = decay * row_gain[None, :, None] * column_gain[None, None, :]
    base = jnp.clip(jax.random.normal(first_key, (2, 3, Z, Y, X), jnp.float32), -4.0, 4.0)
    return (base * amplitude[None, None, :, :, :]).astype(jnp.bfloat16)


def setup_inputs(seed: int = 0) -> dict:
    splits = jax.random.split(jax.random.key(seed), 3)
    state = draw_state(jax.random.fold_in(splits[2], 71), 0)
    shells = draw_shells(jax.random.fold_in(splits[2], 71), 0)
    return {"state": state, "shells": shells}


def reference(state, shells):
    restored = state.astype(jnp.float32)
    energy = 0.5 * jnp.sum(restored * restored, axis=(0, 1))
    totals = jax.ops.segment_sum(energy.reshape(-1), shells.reshape(-1).astype(jnp.int32), num_segments=SHELLS)
    spectrum = totals * (SHELLS / (Z * Y * X))
    return restored, spectrum
```

```python
import functools

import jax
import jax.numpy as jnp
from jax import lax
from jax.experimental import pallas as pl
from jax.experimental.pallas import tpu as pltpu
from jax.sharding import PartitionSpec as P

SHELLS = 512
LOW = 32
HIGH = SHELLS // LOW
LANES = 128
SPEC_ROWS = SHELLS // LANES
GROUP_ROWS = 16
MESH = pl.DeviceIdType.MESH


def kernel(
    slab_count,
    py_count,
    px_count,
    state,
    shells,
    out,
    spec,
    modes,
    labels,
    slab_parts,
    group_parts,
    state_sem,
    label_sem,
    own_sem,
    send_sem,
    recv_sem,
    slab_send,
    slab_recv,
    part_send,
    part_recv,
):
    slab = lax.axis_index("slab")
    py = lax.axis_index("py")
    px = lax.axis_index("px")
    group = py_count * px_count
    me = py * px_count + px
    _, _, planes, rows, columns = state.shape
    planes_out = planes // py_count
    columns_out = columns // px_count

    def load_state(z):
        return pltpu.make_async_copy(state.at[:, :, z], modes.at[:, :, z], state_sem.at[z])

    def load_labels(z):
        return pltpu.make_async_copy(shells.at[z], labels.at[z], label_sem.at[z])

    def group_peer(step):
        peer = lax.rem(me + step, group)
        return (peer, peer // px_count, lax.rem(peer, px_count))

    def slab_peer(step):
        return lax.rem(slab + step, slab_count)

    def block(source, dest_py, dest_px):
        return source.at[
            :,
            :,
            pl.ds(dest_py * planes_out, planes_out),
            :,
            pl.ds(pl.multiple_of(dest_px * columns_out, columns_out), columns_out),
        ]

    def landing(source):
        return out.at[:, :, :, pl.ds(pl.multiple_of(source * rows, rows), rows), :]

    def send_block(dest_py, dest_px):
        return pltpu.make_async_remote_copy(
            src_ref=block(state, dest_py, dest_px),
            dst_ref=landing(me),
            send_sem=send_sem.at[dest_py * px_count + dest_px],
            recv_sem=recv_sem.at[me],
            device_id=(slab, dest_py, dest_px),
            device_id_type=MESH,
        )

    def take_block(source, source_py, source_px):
        return pltpu.make_async_remote_copy(
            src_ref=block(state, source_py, source_px),
            dst_ref=landing(source),
            send_sem=send_sem.at[source],
            recv_sem=recv_sem.at[source],
            device_id=(slab, source_py, source_px),
            device_id_type=MESH,
        )

    def send_at(distance):
        for turn in range(py_count):
            dest_py = lax.rem(py + turn, py_count)
            if distance == 0:
                if turn > 0:
                    send_block(dest_py, px).start()
                continue

            @pl.when(px + distance < px_count)
            def _():
                send_block(dest_py, px + distance).start()

            @pl.when(px - distance >= 0)
            def _():
                send_block(dest_py, px - distance).start()

    def slab_copy(dest, slot):
        return pltpu.make_async_remote_copy(
            src_ref=slab_parts.at[slab],
            dst_ref=slab_parts.at[slot],
            send_sem=slab_send.at[dest],
            recv_sem=slab_recv.at[slot],
            device_id=(dest, py, px),
            device_id_type=MESH,
        )

    def part_copy(dest, dest_py, dest_px, slot):
        return pltpu.make_async_remote_copy(
            src_ref=group_parts.at[me],
            dst_ref=group_parts.at[slot],
            send_sem=part_send.at[dest],
            recv_sem=part_recv.at[slot],
            device_id=(slab, dest_py, dest_px),
            device_id_type=MESH,
        )

    for z in range(planes):
        load_state(z).start()
        load_labels(z).start()

    barrier = pltpu.get_barrier_semaphore()
    for step in range(1, group):
        _, peer_py, peer_px = group_peer(step)
        pl.semaphore_signal(
            barrier, inc=1, device_id=(slab, peer_py, peer_px), device_id_type=MESH
        )
    for step in range(1, slab_count):
        pl.semaphore_signal(
            barrier, inc=1, device_id=(slab_peer(step), py, px), device_id_type=MESH
        )
    pl.semaphore_wait(barrier, group - 1 + slab_count - 1)

    for distance in range(px_count - 1):
        send_at(distance)

    low_ids = lax.broadcasted_iota(jnp.int32, (LOW, columns), 0)
    high_ids = lax.broadcasted_iota(jnp.int32, (HIGH, columns), 0)

    def add_rows(z, start, running):
        values = modes[:, :, z, pl.ds(start, GROUP_ROWS), :].astype(jnp.float32)
        energy = 0.5 * jnp.sum(values * values, axis=(0, 1))
        upper = energy.astype(jnp.bfloat16).astype(jnp.float32)
        lower = energy - upper
        numbers = labels[z, pl.ds(start, GROUP_ROWS), :]
        high = numbers >> (LOW.bit_length() - 1)
        low = numbers & (LOW - 1)
        for row in range(GROUP_ROWS):
            one = slice(row, row + 1)
            hot = high_ids == high[one]
            weighted = jnp.concatenate(
                [jnp.where(hot, upper[one], 0.0), jnp.where(hot, lower[one], 0.0)], axis=0
            ).astype(jnp.bfloat16)
            onehot = jnp.where(low_ids == low[one], 1.0, 0.0).astype(jnp.bfloat16)
            running = running + lax.dot_general(
                weighted, onehot, (((1,), (1,)), ((), ())), preferred_element_type=jnp.float32
            )
        return running

    running = jnp.zeros((2 * HIGH, LOW), jnp.float32)
    for z in range(planes):
        load_state(z).wait()
        load_labels(z).wait()

    own = pltpu.make_async_copy(block(modes, py, px), landing(me), own_sem)
    own.start()

    groups = rows // GROUP_ROWS
    running = lax.fori_loop(
        0,
        planes * groups,
        lambda i, total: add_rows(
            i // groups, pl.multiple_of(lax.rem(i, groups) * GROUP_ROWS, GROUP_ROWS), total
        ),
        running,
    )
    part = running[:HIGH] + running[HIGH:]
    per_row = LANES // LOW
    for high in range(HIGH):
        lane = (high % per_row) * LOW
        slab_parts[slab, high // per_row : high // per_row + 1, lane : lane + LOW] = part[
            high : high + 1
        ]

    for step in range(1, slab_count):
        slab_copy(slab_peer(step), slab).start()
    for step in range(1, slab_count):
        slab_copy(slab_peer(step), slab_peer(step)).wait_recv()
    total = slab_parts[0]
    for slot in range(1, slab_count):
        total = total + slab_parts[slot]
    group_parts[me] = total
    for step in range(1, group):
        part_copy(*group_peer(step), me).start()

    send_at(px_count - 1)

    for step in range(1, group):
        peer, peer_py, peer_px = group_peer(step)
        part_copy(peer, peer_py, peer_px, peer).wait_recv()
    total = group_parts[0]
    for slot in range(1, group):
        total = total + group_parts[slot]
    spec[...] = total

    own.wait()
    for step in range(1, slab_count):
        slab_copy(slab_peer(step), slab).wait_send()
    for step in range(1, group):
        peer, peer_py, peer_px = group_peer(step)
        part_copy(peer, peer_py, peer_px, me).wait_send()
        send_block(peer_py, peer_px).wait_send()
        take_block(peer, peer_py, peer_px).wait_recv()


def local(state, shells):
    slab_count = lax.axis_size("slab")
    py_count = lax.axis_size("py")
    px_count = lax.axis_size("px")
    group = py_count * px_count
    _, _, planes, rows, columns = state.shape
    moved, totals = pl.pallas_call(
        functools.partial(kernel, slab_count, py_count, px_count),
        out_shape=(
            jax.ShapeDtypeStruct(
                (2, 3, planes // py_count, rows * group, columns // px_count), state.dtype
            ),
            jax.ShapeDtypeStruct((SPEC_ROWS, LANES), jnp.float32),
        ),
        in_specs=[pl.BlockSpec(memory_space=pl.ANY)] * 2,
        out_specs=(
            pl.BlockSpec(memory_space=pl.ANY),
            pl.BlockSpec(memory_space=pltpu.VMEM),
        ),
        scratch_shapes=[
            pltpu.VMEM(state.shape, state.dtype),
            pltpu.VMEM(shells.shape, shells.dtype),
            pltpu.VMEM((slab_count, SPEC_ROWS, LANES), jnp.float32),
            pltpu.VMEM((group, SPEC_ROWS, LANES), jnp.float32),
            pltpu.SemaphoreType.DMA((planes,)),
            pltpu.SemaphoreType.DMA((planes,)),
            pltpu.SemaphoreType.DMA,
            pltpu.SemaphoreType.DMA((group,)),
            pltpu.SemaphoreType.DMA((group,)),
            pltpu.SemaphoreType.DMA((slab_count,)),
            pltpu.SemaphoreType.DMA((slab_count,)),
            pltpu.SemaphoreType.DMA((group,)),
            pltpu.SemaphoreType.DMA((group,)),
        ],
        compiler_params=pltpu.CompilerParams(collective_id=0, has_side_effects=True),
    )(state, shells)
    modes_all = planes * rows * columns * slab_count * group
    spectrum = totals.reshape(SHELLS) * (SHELLS / modes_all)
    return (moved.astype(jnp.float32), spectrum)


def solution(mesh):
    return jax.shard_map(
        local,
        mesh=mesh,
        in_specs=(P(None, None, "slab", ("py", "px"), None), P("slab", ("py", "px"), None)),
        out_specs=(P(None, None, ("slab", "py"), None, "px"), P()),
        check_vma=False,
    )
```

```python
import functools

import jax
import jax.numpy as jnp
from jax import lax
from jax.experimental import pallas as pl
from jax.experimental.pallas import tpu as pltpu
from jax.sharding import PartitionSpec as P

SHELLS = 512
LOW = 32
HIGH = SHELLS // LOW
LANES = 128
SPEC_ROWS = SHELLS // LANES
GROUP_ROWS = 16
MESH = pl.DeviceIdType.MESH


def kernel(
    slab_count,
    py_count,
    px_count,
    state,
    shells,
    out,
    spec,
    modes,
    labels,
    slab_parts,
    group_parts,
    state_sem,
    label_sem,
    own_sem,
    send_sem,
    recv_sem,
    slab_send,
    slab_recv,
    part_send,
    part_recv,
):
    slab = lax.axis_index("slab")
    py = lax.axis_index("py")
    px = lax.axis_index("px")
    group = py_count * px_count
    me = py * px_count + px
    _, _, planes, rows, columns = state.shape
    planes_out = planes // py_count
    columns_out = columns // px_count

    def load_state(z):
        return pltpu.make_async_copy(state.at[:, :, z], modes.at[:, :, z], state_sem.at[z])

    def load_labels(z):
        return pltpu.make_async_copy(shells.at[z], labels.at[z], label_sem.at[z])

    def group_peer(step):
        peer = lax.rem(me + step, group)
        return (peer, peer // px_count, lax.rem(peer, px_count))

    def slab_peer(step):
        return lax.rem(slab + step, slab_count)

    def block(source, dest_py, dest_px):
        return source.at[
            :,
            :,
            pl.ds(dest_py * planes_out, planes_out),
            :,
            pl.ds(pl.multiple_of(dest_px * columns_out, columns_out), columns_out),
        ]

    def landing(source):
        return out.at[:, :, :, pl.ds(pl.multiple_of(source * rows, rows), rows), :]

    def send_block(dest_py, dest_px):
        return pltpu.make_async_remote_copy(
            src_ref=block(state, dest_py, dest_px),
            dst_ref=landing(me),
            send_sem=send_sem.at[dest_py * px_count + dest_px],
            recv_sem=recv_sem.at[me],
            device_id=(slab, dest_py, dest_px),
            device_id_type=MESH,
        )

    def take_block(source, source_py, source_px):
        return pltpu.make_async_remote_copy(
            src_ref=block(state, source_py, source_px),
            dst_ref=landing(source),
            send_sem=send_sem.at[source],
            recv_sem=recv_sem.at[source],
            device_id=(slab, source_py, source_px),
            device_id_type=MESH,
        )

    def send_at(distance):
        for turn in range(py_count):
            dest_py = lax.rem(py + turn, py_count)
            if distance == 0:
                if turn > 0:
                    send_block(dest_py, px).start()
                continue

            @pl.when(px + distance < px_count)
            def _():
                send_block(dest_py, px + distance).start()

            @pl.when(px - distance >= 0)
            def _():
                send_block(dest_py, px - distance).start()

    def slab_copy(dest, slot):
        return pltpu.make_async_remote_copy(
            src_ref=slab_parts.at[slab],
            dst_ref=slab_parts.at[slot],
            send_sem=slab_send.at[dest],
            recv_sem=slab_recv.at[slot],
            device_id=(dest, py, px),
            device_id_type=MESH,
        )

    def part_copy(dest, dest_py, dest_px, slot):
        return pltpu.make_async_remote_copy(
            src_ref=group_parts.at[me],
            dst_ref=group_parts.at[slot],
            send_sem=part_send.at[dest],
            recv_sem=part_recv.at[slot],
            device_id=(slab, dest_py, dest_px),
            device_id_type=MESH,
        )

    for z in range(planes):
        load_state(z).start()
        load_labels(z).start()

    barrier = pltpu.get_barrier_semaphore()
    for step in range(1, group):
        _, peer_py, peer_px = group_peer(step)
        pl.semaphore_signal(
            barrier, inc=1, device_id=(slab, peer_py, peer_px), device_id_type=MESH
        )
    for step in range(1, slab_count):
        pl.semaphore_signal(
            barrier, inc=1, device_id=(slab_peer(step), py, px), device_id_type=MESH
        )
    pl.semaphore_wait(barrier, group - 1 + slab_count - 1)

    for distance in range(px_count - 1, 0, -1):
        send_at(distance)

    low_ids = lax.broadcasted_iota(jnp.int32, (LOW, columns), 0)
    high_ids = lax.broadcasted_iota(jnp.int32, (HIGH, columns), 0)

    def add_rows(z, start, running):
        values = modes[:, :, z, pl.ds(start, GROUP_ROWS), :].astype(jnp.float32)
        energy = 0.5 * jnp.sum(values * values, axis=(0, 1))
        upper = energy.astype(jnp.bfloat16).astype(jnp.float32)
        lower = energy - upper
        numbers = labels[z, pl.ds(start, GROUP_ROWS), :]
        high = numbers >> (LOW.bit_length() - 1)
        low = numbers & (LOW - 1)
        for row in range(GROUP_ROWS):
            one = slice(row, row + 1)
            hot = high_ids == high[one]
            weighted = jnp.concatenate(
                [jnp.where(hot, upper[one], 0.0), jnp.where(hot, lower[one], 0.0)], axis=0
            ).astype(jnp.bfloat16)
            onehot = jnp.where(low_ids == low[one], 1.0, 0.0).astype(jnp.bfloat16)
            running = running + lax.dot_general(
                weighted, onehot, (((1,), (1,)), ((), ())), preferred_element_type=jnp.float32
            )
        return running

    running = jnp.zeros((2 * HIGH, LOW), jnp.float32)
    for z in range(planes):
        load_state(z).wait()
        load_labels(z).wait()

    own = pltpu.make_async_copy(block(state, py, px), landing(me), own_sem)
    own.start()

    groups = rows // GROUP_ROWS
    running = lax.fori_loop(
        0,
        planes * groups,
        lambda i, total: add_rows(
            i // groups, pl.multiple_of(lax.rem(i, groups) * GROUP_ROWS, GROUP_ROWS), total
        ),
        running,
    )
    part = running[:HIGH] + running[HIGH:]
    per_row = LANES // LOW
    for high in range(HIGH):
        lane = (high % per_row) * LOW
        slab_parts[slab, high // per_row : high // per_row + 1, lane : lane + LOW] = part[
            high : high + 1
        ]

    for step in range(1, slab_count):
        slab_copy(slab_peer(step), slab).start()
    for step in range(1, slab_count):
        slab_copy(slab_peer(step), slab_peer(step)).wait_recv()
    total = slab_parts[0]
    for slot in range(1, slab_count):
        total = total + slab_parts[slot]
    group_parts[me] = total
    for step in range(1, group):
        part_copy(*group_peer(step), me).start()

    send_at(0)

    for step in range(1, group):
        peer, peer_py, peer_px = group_peer(step)
        part_copy(peer, peer_py, peer_px, peer).wait_recv()
    total = group_parts[0]
    for slot in range(1, group):
        total = total + group_parts[slot]
    spec[...] = total

    own.wait()
    for step in range(1, slab_count):
        slab_copy(slab_peer(step), slab).wait_send()
    for step in range(1, group):
        peer, peer_py, peer_px = group_peer(step)
        part_copy(peer, peer_py, peer_px, me).wait_send()
        send_block(peer_py, peer_px).wait_send()
        take_block(peer, peer_py, peer_px).wait_recv()


def local(state, shells):
    slab_count = lax.axis_size("slab")
    py_count = lax.axis_size("py")
    px_count = lax.axis_size("px")
    group = py_count * px_count
    _, _, planes, rows, columns = state.shape
    moved, totals = pl.pallas_call(
        functools.partial(kernel, slab_count, py_count, px_count),
        out_shape=(
            pltpu.VMEM(
                (2, 3, planes // py_count, rows * group, columns // px_count), state.dtype
            ),
            jax.ShapeDtypeStruct((SPEC_ROWS, LANES), jnp.float32),
        ),
        in_specs=[pl.BlockSpec(memory_space=pl.ANY)] * 2,
        out_specs=(
            pl.BlockSpec(memory_space=pltpu.VMEM),
            pl.BlockSpec(memory_space=pltpu.VMEM),
        ),
        scratch_shapes=[
            pltpu.VMEM(state.shape, state.dtype),
            pltpu.VMEM(shells.shape, shells.dtype),
            pltpu.VMEM((slab_count, SPEC_ROWS, LANES), jnp.float32),
            pltpu.VMEM((group, SPEC_ROWS, LANES), jnp.float32),
            pltpu.SemaphoreType.DMA((planes,)),
            pltpu.SemaphoreType.DMA((planes,)),
            pltpu.SemaphoreType.DMA,
            pltpu.SemaphoreType.DMA((group,)),
            pltpu.SemaphoreType.DMA((group,)),
            pltpu.SemaphoreType.DMA((slab_count,)),
            pltpu.SemaphoreType.DMA((slab_count,)),
            pltpu.SemaphoreType.DMA((group,)),
            pltpu.SemaphoreType.DMA((group,)),
        ],
        compiler_params=pltpu.CompilerParams(collective_id=0, has_side_effects=True, vmem_limit_bytes=24 << 20),
    )(
        pltpu.with_memory_space_constraint(state, pltpu.HBM),
        pltpu.with_memory_space_constraint(shells, pltpu.HBM),
    )
    modes_all = planes * rows * columns * slab_count * group
    spectrum = totals.reshape(SHELLS) * (SHELLS / modes_all)
    return (moved.astype(jnp.float32), spectrum)


def solution(mesh):
    return jax.shard_map(
        local,
        mesh=mesh,
        in_specs=(P(None, None, "slab", ("py", "px"), None), P("slab", ("py", "px"), None)),
        out_specs=(P(None, None, ("slab", "py"), None, "px"), P()),
        check_vma=False,
    )
```
